32 devices in a mesh: grp: 2 (over y), fib: 4 (over z), wav: 2 (over x), arm: 2 (over core).
Axes of the slice: x: 2, y: 2, z: 4, core: 2. Of those that a mesh axis runs over, the one named last changes fastest.
Arguments:
- spectra: bfloat16 [32, 2, 2, 128, 256], P(('grp', 'fib'), 'arm', None, None, 'wav'), parts along dimension 0, as said below
- bands: bfloat16 [32, 2, 11, 128, 256], P(('grp', 'fib'), 'arm', None, None, 'wav'), parts along dimension 0, may hold values from 0 to 0.29882812
- coverage: int32 [32, 128], P(('grp', 'fib')), parts along dimension 0, may hold values from 0 to 1, as said below
Outputs:
- flux_coadd: float32 [2, 256, 256], P('arm', ('grp', 'fib'), 'wav'), parts along dimension 1
- ivar_coadd: float32 [2, 256, 256], P('arm', ('grp', 'fib'), 'wav'), parts along dimension 1
- res_coadd: float32 [2, 11, 256, 256], P('arm', None, ('grp', 'fib'), 'wav'), parts along dimension 2
- model: float32 [2, 256, 256], P('arm', ('grp', 'fib'), 'wav'), parts along dimension 1
The draws below stay inside these ranges and needn't reach their ends.
There are 2 independent parts, one for each index of `grp`. The reference program is written for one: setup_inputs(seed, part) draws one part's arguments, and reference() takes and returns one part's arrays. A program takes and returns all parts, laid end to end along the dimension named above; each array names one. Nothing has to cross between parts.
Inputs may be any that keep to these rules, and one draw needn't show every extreme that they name: `spectra`: channel 1 (inverse variance) lies between 0.25 and 4. `coverage`: every fiber is observed by at least one exposure.
All inputs are finite; a program needn't handle non-finite values.
Results may differ from the reference program's by a relative error of at most 0.0003.
Values may be sent and summed in bfloat16 or wider, within the bound.
A program may use at most 64 MiB of HBM per device.

```python
import math
import jax
import jax.numpy as jnp
from jax import lax

BANDS = 11
EXPOSURES = 16
FIBERS = 128
WAVES = 256
ARMS = 2


def draw_spectra(key, part):
    key_sig, key_noise, key_ivar, key_mean = jax.random.split(jax.random.fold_in(key, 11), 4)
    signal = jax.random.normal(key_sig, (1, ARMS, FIBERS, WAVES), jnp.float32)
    shape = (EXPOSURES, ARMS, FIBERS, WAVES)
    ivar = jnp.exp(jax.random.uniform(key_ivar, shape, jnp.float32, math.log(0.25), math.log(4.0)))
    noise = jax.random.normal(key_noise, shape, jnp.float32) * lax_rsqrt(ivar)
    flux = signal + noise
    return jnp.stack([flux, ivar], 2).astype(jnp.bfloat16)


def lax_rsqrt(values):
    return 1.0 / jnp.sqrt(values)


def draw_coverage(key, part):
    key_level, key_roll = jax.random.split(jax.random.fold_in(key, 7))
    level = jax.random.randint(key_level, (1, FIBERS), 1, 5)
    roll = jax.random.randint(key_roll, (EXPOSURES, FIBERS), 0, 4)
    expo = jnp.arange(EXPOSURES, dtype=jnp.int32)[:, None]
    fiber = jnp.arange(FIBERS, dtype=jnp.int32)[None, :]
    forced = expo == fiber % EXPOSURES
    return jnp.where((roll < level) | forced, 1, 0).astype(jnp.int32)


def steps_of(own_key, shape, cuts, smallest, top_value):
    loudness = 1.0
    for dim, parts in cuts:
        steps = jax.random.uniform(jax.random.fold_in(jax.random.fold_in(own_key, 6), dim), (parts,), jnp.float32, smallest / len(cuts), top_value / len(cuts))
        loudness = loudness * jnp.repeat(jnp.exp(steps), shape[dim] // parts).reshape((-1,) + (1,) * (len(shape) - 1 - dim))
    return loudness


def setup_inputs(seed: int = 0, part: int = 0) -> dict:
    keys = jax.random.split(jax.random.key(seed), 4)
    part_splits = jax.random.split(jax.random.fold_in(keys[3], part), 4)
    spectra = draw_spectra(jax.random.fold_in(jax.random.fold_in(keys[3], part), 71), part)
    bands = jnp.clip(0.29882812 * jax.random.uniform(part_splits[1], (EXPOSURES, ARMS, BANDS, FIBERS, WAVES), jnp.float32) ** steps_of(part_splits[1], (EXPOSURES, ARMS, BANDS, FIBERS, WAVES), ((0, 4), (1, 2), (4, 2)), -0.2, 0.2), 0.0, 0.29882812).astype(jnp.bfloat16)
    coverage = draw_coverage(jax.random.fold_in(jax.random.fold_in(keys[3], part), 71), part)
    return {"spectra": spectra, "bands": bands, "coverage": coverage}


def reference(spectra, bands, coverage):
    coverage_bf = coverage.astype(jnp.bfloat16)[:, None, :, None]
    weights = spectra[:, :, 1] * coverage_bf

    def accumulate(carry, items):
        weight_one, flux_one, band_one = items
        weight_one = weight_one.astype(jnp.float32)
        return (carry[0] + weight_one,
                carry[1] + weight_one * flux_one.astype(jnp.float32),
                carry[2] + weight_one[:, None] * band_one.astype(jnp.float32)), None

    arms, fibers, waves = weights.shape[1], weights.shape[2], weights.shape[3]
    nbands = bands.shape[2]
    start = (jnp.zeros((arms, fibers, waves), jnp.float32),
             jnp.zeros((arms, fibers, waves), jnp.float32),
             jnp.zeros((arms, nbands, fibers, waves), jnp.float32))
    (ivar_coadd, flux_sum, band_sum), _ = lax.scan(accumulate, start, (weights, spectra[:, :, 0], bands))
    flux_coadd = flux_sum / ivar_coadd
    res_coadd = band_sum / ivar_coadd[:, None]
    padded = jnp.pad(flux_coadd, ((0, 0), (0, 0), (5, 5)))
    model = res_coadd[:, 0] * padded[:, :, 0:waves]
    for band_idx in range(1, nbands):
        model = model + res_coadd[:, band_idx] * padded[:, :, band_idx:band_idx + waves]
    return flux_coadd, ivar_coadd, res_coadd, model
```

```python
import functools

import jax
import jax.numpy as jnp
from jax import lax
from jax.experimental import pallas as pl
from jax.experimental.pallas import tpu as pltpu
from jax.sharding import PartitionSpec as P

MESH = pl.DeviceIdType.MESH
HALF = 5
UNIT = 512.0
TOP = 32767.0
TINY = 1e-30
ROWS = 16


def kernel(n_fib, n_wav, spec_hbm, bands_hbm, cov_hbm, flux_out, ivar_out, res_out, model_out,
           spec, bands, cov, weight, flux_send, ivar_send, scale_send, band_send,
           flux_recv, ivar_recv, scale_recv, band_recv, own_band, flux_full, side, rolled,
           load_sem, send_sem, recv_sem, side_send_sem, side_recv_sem):
    f32 = jnp.float32
    me = lax.axis_index("fib")
    w_me = lax.axis_index("wav")
    right, left = lax.rem(w_me + 1, n_wav), lax.rem(w_me + n_wav - 1, n_wav)
    exposures, n_bands, fibers, width = bands.shape
    share = fibers // n_fib

    cov_load = pltpu.make_async_copy(cov_hbm, cov, load_sem.at[0])
    spec_load = pltpu.make_async_copy(spec_hbm, spec, load_sem.at[1])
    band_load = pltpu.make_async_copy(bands_hbm, bands, load_sem.at[2])
    cov_load.start()
    spec_load.start()
    band_load.start()

    def peer(t):
        low = n_fib - 1 - t
        low = jnp.where(low <= me, low - 1, low)
        high = jnp.where(t >= me, t + 1, t)
        return jnp.where(2 * me < n_fib, low, high)

    barrier = pltpu.get_barrier_semaphore()

    def greet(t, c):
        pl.semaphore_signal(barrier, inc=1, device_id={"fib": peer(t)}, device_id_type=MESH)
        return c

    lax.fori_loop(0, n_fib - 1, greet, 0)
    pl.semaphore_signal(barrier, inc=1, device_id={"wav": right}, device_id_type=MESH)
    pl.semaphore_signal(barrier, inc=1, device_id={"wav": left}, device_id_type=MESH)

    cov_load.wait()
    spec_load.wait()

    seen = cov[...].astype(f32)
    for e in range(exposures):
        column = jnp.transpose(jnp.broadcast_to(seen[e : e + 1, :], (width, fibers)))
        weight[e] = spec[e, 1].astype(f32) * column

    def head(d):
        rows = pl.ds(pl.multiple_of(d * share, share), share)
        w = [weight[e, rows, :] for e in range(exposures)]
        ivar = w[0]
        flux = w[0] * spec[0, 0, rows, :].astype(f32)
        for e in range(1, exposures):
            ivar += w[e]
            flux += w[e] * spec[e, 0, rows, :].astype(f32)
        return ivar, flux

    def copies(kind, t):
        src, dst = ((flux_send, flux_recv), (ivar_send, ivar_recv),
                    (scale_send, scale_recv), (band_send, band_recv))[kind]
        d = peer(t)
        return pltpu.make_async_remote_copy(
            src_ref=src.at[d], dst_ref=dst.at[me], send_sem=send_sem.at[kind, d],
            recv_sem=recv_sem.at[kind, me], device_id={"fib": d}, device_id_type=MESH)

    def arrival(kind, t):
        src, dst = ((flux_send, flux_recv), (ivar_send, ivar_recv),
                    (scale_send, scale_recv), (band_send, band_recv))[kind]
        d = peer(t)
        return pltpu.make_async_remote_copy(
            src_ref=src.at[d], dst_ref=dst.at[d], send_sem=send_sem.at[kind, d],
            recv_sem=recv_sem.at[kind, d], device_id={"fib": d}, device_id_type=MESH)

    def make_head(t, c):
        d = peer(t)
        ivar, flux = head(d)
        flux_send[d] = flux
        ivar_send[d] = (ivar * UNIT).astype(jnp.int32).astype(jnp.int16)
        return c

    lax.fori_loop(0, n_fib - 1, make_head, 0)
    pl.semaphore_wait(barrier, n_fib + 1)

    def send_head(t, c):
        copies(0, t).start()
        copies(1, t).start()
        return c

    lax.fori_loop(0, n_fib - 1, send_head, 0)
    band_load.wait()

    def sums(d, j):
        rows = pl.ds(pl.multiple_of(d * share + j * ROWS, ROWS), ROWS)
        w = [weight[e, rows, :] for e in range(exposures)]
        out = []
        for b in range(n_bands):
            total = w[0] * bands[0, b, rows, :].astype(f32)
            for e in range(1, exposures):
                total += w[e] * bands[e, b, rows, :].astype(f32)
            out.append(total)
        return out

    def make_bands(t, c):
        d = peer(t)
        for j in range(share // ROWS):
            piece = pl.ds(j * ROWS, ROWS)
            total = sums(d, j)
            top = functools.reduce(jnp.maximum, total)
            scale = (jnp.maximum(top, TINY) * 1.01).astype(jnp.bfloat16)
            scale_send[d, piece, :] = scale
            factor = TOP / scale.astype(f32)
            for b in range(n_bands):
                band_send[d, b, piece, :] = (total[b] * factor + 0.5).astype(jnp.int32).astype(jnp.int16)
        copies(2, t).start()
        copies(3, t).start()
        return c

    lax.fori_loop(0, n_fib - 1, make_bands, 0)

    for j in range(share // ROWS):
        total = sums(me, j)
        for b in range(n_bands):
            own_band[b, pl.ds(j * ROWS, ROWS), :] = total[b]
    ivar, flux = head(me)

    def add_head(t, carry):
        ivar, flux = carry
        d = peer(n_fib - 2 - t)
        arrival(0, n_fib - 2 - t).wait_recv()
        arrival(1, n_fib - 2 - t).wait_recv()
        return ivar + ivar_recv[d].astype(f32) * (1.0 / UNIT), flux + flux_recv[d]

    ivar, flux = lax.fori_loop(0, n_fib - 1, add_head, (ivar, flux))
    inverse = 1.0 / ivar
    coadd = flux / ivar
    ivar_out[...] = ivar[None]
    flux_out[...] = coadd[None]
    flux_full[...] = coadd
    to_right = pltpu.make_async_remote_copy(
        src_ref=flux_full, dst_ref=side.at[0], send_sem=side_send_sem.at[0], recv_sem=side_recv_sem.at[0],
        device_id={"wav": right}, device_id_type=MESH)
    to_left = pltpu.make_async_remote_copy(
        src_ref=flux_full, dst_ref=side.at[1], send_sem=side_send_sem.at[1], recv_sem=side_recv_sem.at[1],
        device_id={"wav": left}, device_id_type=MESH)
    to_right.start()
    to_left.start()
    to_right.wait_recv()
    to_left.wait_recv()
    before = jnp.where(w_me == 0, 0.0, side[0])
    after = jnp.where(w_me == n_wav - 1, 0.0, side[1])
    lane = lax.broadcasted_iota(jnp.int32, (share, width), 1)
    for b in range(n_bands):
        shift = b - HALF
        if shift == 0:
            rolled[b] = coadd
        elif shift > 0:
            rolled[b] = pltpu.roll(jnp.where(lane >= shift, coadd, after), width - shift, 1)
        else:
            rolled[b] = pltpu.roll(jnp.where(lane < width + shift, coadd, before), -shift, 1)

    def add_bands(t, c):
        d = peer(n_fib - 2 - t)
        arrival(2, n_fib - 2 - t).wait_recv()
        arrival(3, n_fib - 2 - t).wait_recv()
        scale = scale_recv[d].astype(f32) * (1.0 / TOP)
        for b in range(n_bands):
            own_band[b] += band_recv[d, b].astype(f32) * scale
        return c

    lax.fori_loop(0, n_fib - 1, add_bands, 0)
    model = None
    for b in range(n_bands):
        res = own_band[b] * inverse
        res_out[0, b] = res
        term = res * rolled[b]
        model = term if model is None else model + term
    model_out[...] = model[None]

    def finish(t, c):
        for kind in range(4):
            copies(kind, t).wait_send()
        return c

    lax.fori_loop(0, n_fib - 1, finish, 0)
    to_right.wait_send()
    to_left.wait_send()


def local(n_fib, n_wav, spectra, bands, coverage):
    spectra, bands = spectra[:, 0], bands[:, 0]
    exposures, n_bands, fibers, width = bands.shape
    share = fibers // n_fib
    f32, i16, bf16 = jnp.float32, jnp.int16, jnp.bfloat16
    plane = jax.ShapeDtypeStruct((1, share, width), f32)
    vmem = pltpu.VMEM
    sem = pltpu.SemaphoreType.DMA
    return pl.pallas_call(
        functools.partial(kernel, n_fib, n_wav),
        out_shape=(plane, plane, jax.ShapeDtypeStruct((1, n_bands, share, width), f32), plane),
        in_specs=[pl.BlockSpec(memory_space=pl.ANY)] * 3,
        out_specs=[pl.BlockSpec(memory_space=pltpu.VMEM)] * 4,
        scratch_shapes=[
            vmem(spectra.shape, bf16),
            vmem(bands.shape, bf16),
            vmem(coverage.shape, jnp.int32),
            vmem((exposures, fibers, width), f32),
            vmem((n_fib, share, width), f32),
            vmem((n_fib, share, width), i16),
            vmem((n_fib, share, width), bf16),
            vmem((n_fib, n_bands, share, width), i16),
            vmem((n_fib, share, width), f32),
            vmem((n_fib, share, width), i16),
            vmem((n_fib, share, width), bf16),
            vmem((n_fib, n_bands, share, width), i16),
            vmem((n_bands, share, width), f32),
            vmem((share, width), f32),
            vmem((2, share, width), f32),
            vmem((n_bands, share, width), f32),
            sem((3,)),
            sem((4, n_fib)),
            sem((4, n_fib)),
            sem((2,)),
            sem((2,)),
        ],
        compiler_params=pltpu.CompilerParams(collective_id=0, has_side_effects=True),
        name="coadd",
    )(spectra, bands, coverage)


def solution(mesh):
    sizes = dict(mesh.shape)
    return jax.shard_map(
        functools.partial(local, sizes["fib"], sizes["wav"]),
        mesh=mesh,
        in_specs=(
            P(("grp", "fib"), "arm", None, None, "wav"),
            P(("grp", "fib"), "arm", None, None, "wav"),
            P(("grp", "fib"), None),
        ),
        out_specs=(
            P("arm", ("grp", "fib"), "wav"),
            P("arm", ("grp", "fib"), "wav"),
            P("arm", None, ("grp", "fib"), "wav"),
            P("arm", ("grp", "fib"), "wav"),
        ),
        check_vma=False,
    )
```

```python
import functools

import jax
import jax.numpy as jnp
from jax import lax
from jax.experimental import pallas as pl
from jax.experimental.pallas import tpu as pltpu
from jax.sharding import PartitionSpec as P

MESH = pl.DeviceIdType.MESH
HALF = 5
UNIT = 512.0
TOP = 32767.0
TINY = 1e-30
ROWS = 16


def kernel(n_fib, n_wav, spec_hbm, bands_hbm, cov_hbm, flux_out, ivar_out, res_out, model_out,
           spec, bands, cov, weight, flux_send, ivar_send, scale_send, band_send,
           flux_recv, ivar_recv, scale_recv, band_recv, own_band, flux_full, side, rolled,
           load_sem, send_sem, recv_sem, side_send_sem, side_recv_sem):
    f32 = jnp.float32
    me = lax.axis_index("fib")
    w_me = lax.axis_index("wav")
    right, left = lax.rem(w_me + 1, n_wav), lax.rem(w_me + n_wav - 1, n_wav)
    exposures, n_bands, fibers, width = bands.shape
    share = fibers // n_fib

    cov_load = pltpu.make_async_copy(cov_hbm, cov, load_sem.at[0])
    spec_load = pltpu.make_async_copy(spec_hbm, spec, load_sem.at[1])
    band_load = pltpu.make_async_copy(bands_hbm, bands, load_sem.at[2])
    cov_load.start()
    spec_load.start()
    band_load.start()

    def peer(t):
        low = n_fib - 1 - t
        low = jnp.where(low <= me, low - 1, low)
        high = jnp.where(t >= me, t + 1, t)
        return jnp.where(2 * me < n_fib, low, high)

    barrier = pltpu.get_barrier_semaphore()

    def greet(t, c):
        pl.semaphore_signal(barrier, inc=1, device_id={"fib": peer(t)}, device_id_type=MESH)
        return c

    lax.fori_loop(0, n_fib - 1, greet, 0)
    pl.semaphore_signal(barrier, inc=1, device_id={"wav": right}, device_id_type=MESH)
    pl.semaphore_signal(barrier, inc=1, device_id={"wav": left}, device_id_type=MESH)

    cov_load.wait()
    spec_load.wait()

    seen = cov[...].astype(f32)
    for e in range(exposures):
        column = jnp.transpose(jnp.broadcast_to(seen[e : e + 1, :], (width, fibers)))
        weight[e] = spec[e, 1].astype(f32) * column

    def head(d):
        rows = pl.ds(pl.multiple_of(d * share, share), share)
        w = [weight[e, rows, :] for e in range(exposures)]
        ivar = w[0]
        flux = w[0] * spec[0, 0, rows, :].astype(f32)
        for e in range(1, exposures):
            ivar += w[e]
            flux += w[e] * spec[e, 0, rows, :].astype(f32)
        return ivar, flux

    def copies(kind, t):
        src, dst = ((flux_send, flux_recv), (ivar_send, ivar_recv),
                    (scale_send, scale_recv), (band_send, band_recv))[kind]
        d = peer(t)
        return pltpu.make_async_remote_copy(
            src_ref=src.at[d], dst_ref=dst.at[me], send_sem=send_sem.at[kind, d],
            recv_sem=recv_sem.at[kind, me], device_id={"fib": d}, device_id_type=MESH)

    def arrival(kind, t):
        src, dst = ((flux_send, flux_recv), (ivar_send, ivar_recv),
                    (scale_send, scale_recv), (band_send, band_recv))[kind]
        d = peer(t)
        return pltpu.make_async_remote_copy(
            src_ref=src.at[d], dst_ref=dst.at[d], send_sem=send_sem.at[kind, d],
            recv_sem=recv_sem.at[kind, d], device_id={"fib": d}, device_id_type=MESH)

    def make_head(t, c):
        d = peer(t)
        ivar, flux = head(d)
        flux_send[d] = flux
        ivar_send[d] = (ivar * UNIT).astype(jnp.int32).astype(jnp.int16)
        return c

    lax.fori_loop(0, n_fib - 1, make_head, 0)
    pl.semaphore_wait(barrier, n_fib + 1)

    def send_head(t, c):
        copies(0, t).start()
        copies(1, t).start()
        return c

    lax.fori_loop(0, n_fib - 1, send_head, 0)
    band_load.wait()

    def sums(d, j):
        rows = pl.ds(pl.multiple_of(d * share + j * ROWS, ROWS), ROWS)
        w = [weight[e, rows, :] for e in range(exposures)]
        out = []
        for b in range(n_bands):
            total = w[0] * bands[0, b, rows, :].astype(f32)
            for e in range(1, exposures):
                total += w[e] * bands[e, b, rows, :].astype(f32)
            out.append(total)
        return out

    def make_bands(t, c):
        d = peer(t)
        for j in range(share // ROWS):
            piece = pl.ds(j * ROWS, ROWS)
            total = sums(d, j)
            top = functools.reduce(jnp.maximum, total)
            scale = (jnp.maximum(top, TINY) * 1.01).astype(jnp.bfloat16)
            scale_send[d, piece, :] = scale
            factor = TOP / scale.astype(f32)
            for b in range(n_bands):
                band_send[d, b, piece, :] = (total[b] * factor + 0.5).astype(jnp.int32).astype(jnp.int16)
        copies(2, t).start()
        copies(3, t).start()
        return c

    lax.fori_loop(0, n_fib - 1, make_bands, 0)

    for j in range(share // ROWS):
        total = sums(me, j)
        for b in range(n_bands):
            own_band[b, pl.ds(j * ROWS, ROWS), :] = total[b]
    ivar, flux = head(me)

    def add_head(t, carry):
        ivar, flux = carry
        d = peer(n_fib - 2 - t)
        arrival(0, n_fib - 2 - t).wait_recv()
        arrival(1, n_fib - 2 - t).wait_recv()
        return ivar + ivar_recv[d].astype(f32) * (1.0 / UNIT), flux + flux_recv[d]

    ivar, flux = lax.fori_loop(0, n_fib - 1, add_head, (ivar, flux))
    inverse = 1.0 / ivar
    coadd = flux / ivar
    ivar_out[...] = ivar[None]
    flux_out[...] = coadd[None]
    flux_full[...] = coadd
    to_right = pltpu.make_async_remote_copy(
        src_ref=flux_full, dst_ref=side.at[0], send_sem=side_send_sem.at[0], recv_sem=side_recv_sem.at[0],
        device_id={"wav": right}, device_id_type=MESH)
    to_left = pltpu.make_async_remote_copy(
        src_ref=flux_full, dst_ref=side.at[1], send_sem=side_send_sem.at[1], recv_sem=side_recv_sem.at[1],
        device_id={"wav": left}, device_id_type=MESH)
    to_right.start()
    to_left.start()
    to_right.wait_recv()
    to_left.wait_recv()
    before = jnp.where(w_me == 0, 0.0, side[0])
    after = jnp.where(w_me == n_wav - 1, 0.0, side[1])
    lane = lax.broadcasted_iota(jnp.int32, (share, width), 1)
    for b in range(n_bands):
        shift = b - HALF
        if shift == 0:
            rolled[b] = coadd
        elif shift > 0:
            rolled[b] = pltpu.roll(jnp.where(lane >= shift, coadd, after), width - shift, 1)
        else:
            rolled[b] = pltpu.roll(jnp.where(lane < width + shift, coadd, before), -shift, 1)

    def add_bands(t, c):
        d = peer(n_fib - 2 - t)
        arrival(2, n_fib - 2 - t).wait_recv()
        arrival(3, n_fib - 2 - t).wait_recv()
        scale = scale_recv[d].astype(f32) * (1.0 / TOP)
        for b in range(n_bands):
            own_band[b] += band_recv[d, b].astype(f32) * scale
        return c

    lax.fori_loop(0, n_fib - 1, add_bands, 0)
    model = None
    for b in range(n_bands):
        res = own_band[b] * inverse
        res_out[0, b] = res
        term = res * rolled[b]
        model = term if model is None else model + term
    model_out[...] = model[None]

    def finish(t, c):
        for kind in range(4):
            copies(kind, t).wait_send()
        return c

    lax.fori_loop(0, n_fib - 1, finish, 0)
    to_right.wait_send()
    to_left.wait_send()


def write_out(*refs):
    half = len(refs) // 2
    sem = refs[-1]
    loads = [pltpu.make_async_copy(refs[i], refs[half + i], sem.at[i]) for i in range(half)]
    for copy in loads:
        copy.start()
    for copy in loads:
        copy.wait()


def local(n_fib, n_wav, spectra, bands, coverage):
    spectra, bands = spectra[:, 0], bands[:, 0]
    exposures, n_bands, fibers, width = bands.shape
    share = fibers // n_fib
    f32, i16, bf16 = jnp.float32, jnp.int16, jnp.bfloat16
    plane = jax.ShapeDtypeStruct((1, share, width), f32)
    vmem = pltpu.VMEM
    sem = pltpu.SemaphoreType.DMA
    shapes = (plane, plane, jax.ShapeDtypeStruct((1, n_bands, share, width), f32), plane)
    parts = pl.pallas_call(
        functools.partial(kernel, n_fib, n_wav),
        out_shape=tuple(vmem(x.shape, f32) for x in shapes),
        in_specs=[pl.BlockSpec(memory_space=pl.ANY)] * 3,
        out_specs=[pl.BlockSpec(memory_space=pltpu.VMEM)] * 4,
        scratch_shapes=[
            vmem(spectra.shape, bf16),
            vmem(bands.shape, bf16),
            vmem(coverage.shape, jnp.int32),
            vmem((exposures, fibers, width), f32),
            vmem((n_fib, share, width), f32),
            vmem((n_fib, share, width), i16),
            vmem((n_fib, share, width), bf16),
            vmem((n_fib, n_bands, share, width), i16),
            vmem((n_fib, share, width), f32),
            vmem((n_fib, share, width), i16),
            vmem((n_fib, share, width), bf16),
            vmem((n_fib, n_bands, share, width), i16),
            vmem((n_bands, share, width), f32),
            vmem((share, width), f32),
            vmem((2, share, width), f32),
            vmem((n_bands, share, width), f32),
            sem((3,)),
            sem((4, n_fib)),
            sem((4, n_fib)),
            sem((2,)),
            sem((2,)),
        ],
        compiler_params=pltpu.CompilerParams(collective_id=0, has_side_effects=True),
        name="coadd",
    )(spectra, bands, coverage)
    return pl.pallas_call(
        write_out,
        out_shape=shapes,
        in_specs=[pl.BlockSpec(memory_space=pltpu.VMEM)] * 4,
        out_specs=[pl.BlockSpec(memory_space=pl.ANY)] * 4,
        scratch_shapes=[sem((4,))],
        compiler_params=pltpu.CompilerParams(vmem_limit_bytes=4 * 2**20),
        name="write_out",
    )(*parts)


def solution(mesh):
    sizes = dict(mesh.shape)
    return jax.shard_map(
        functools.partial(local, sizes["fib"], sizes["wav"]),
        mesh=mesh,
        in_specs=(
            P(("grp", "fib"), "arm", None, None, "wav"),
            P(("grp", "fib"), "arm", None, None, "wav"),
            P(("grp", "fib"), None),
        ),
        out_specs=(
            P("arm", ("grp", "fib"), "wav"),
            P("arm", ("grp", "fib"), "wav"),
            P("arm", None, ("grp", "fib"), "wav"),
            P("arm", ("grp", "fib"), "wav"),
        ),
        check_vma=False,
    )
```

```python
import functools

import jax
import jax.numpy as jnp
from jax import lax
from jax.experimental import pallas as pl
from jax.experimental.pallas import tpu as pltpu
from jax.sharding import PartitionSpec as P

MESH = pl.DeviceIdType.MESH
HALF = 5
UNIT = 512.0
TOP = 32767.0
TINY = 1e-30
ROWS = 16


def kernel(n_fib, n_wav, spec_hbm, bands_hbm, cov_hbm, flux_out, ivar_out, res_out, model_out,
           spec, bands, cov, weight, flux_send, ivar_send, scale_send, band_send,
           flux_recv, ivar_recv, scale_recv, band_recv, own_band, held, flux_full, side, rolled,
           load_sem, head_send_sem, head_recv_sem, send_sem, recv_sem, side_send_sem, side_recv_sem):
    f32 = jnp.float32
    me = lax.axis_index("fib")
    w_me = lax.axis_index("wav")
    right, left = lax.rem(w_me + 1, n_wav), lax.rem(w_me + n_wav - 1, n_wav)
    exposures, n_bands, fibers, width = bands.shape
    share = fibers // n_fib

    cov_load = pltpu.make_async_copy(cov_hbm, cov, load_sem.at[0])
    spec_load = pltpu.make_async_copy(spec_hbm, spec, load_sem.at[1])
    band_load = pltpu.make_async_copy(bands_hbm, bands, load_sem.at[2])
    cov_load.start()
    spec_load.start()
    band_load.start()

    def peer(t):
        low = n_fib - 1 - t
        low = jnp.where(low <= me, low - 1, low)
        high = jnp.where(t >= me, t + 1, t)
        return jnp.where(2 * me < n_fib, low, high)

    barrier = pltpu.get_barrier_semaphore()

    def greet(t, c):
        pl.semaphore_signal(barrier, inc=1, device_id={"fib": peer(t)}, device_id_type=MESH)
        return c

    lax.fori_loop(0, n_fib - 1, greet, 0)
    pl.semaphore_signal(barrier, inc=1, device_id={"wav": right}, device_id_type=MESH)
    pl.semaphore_signal(barrier, inc=1, device_id={"wav": left}, device_id_type=MESH)

    cov_load.wait()
    spec_load.wait()

    seen = cov[...].astype(f32)
    for e in range(exposures):
        column = jnp.transpose(jnp.broadcast_to(seen[e : e + 1, :], (width, fibers)))
        weight[e] = spec[e, 1].astype(f32) * column

    pieces = share // ROWS
    is_end = (me == 0) | (me == n_fib - 1)
    is_relay = (me == 1) | (me == n_fib - 2)
    relay = jnp.where(me == 0, 1, n_fib - 2)
    far = jnp.where(me == 1, n_fib - 1, 0)

    def head(d):
        rows = pl.ds(pl.multiple_of(d * share, share), share)
        w = [weight[e, rows, :] for e in range(exposures)]
        ivar = w[0]
        flux = w[0] * spec[0, 0, rows, :].astype(f32)
        for e in range(1, exposures):
            ivar += w[e]
            flux += w[e] * spec[e, 0, rows, :].astype(f32)
        return ivar, flux

    def head_copies(d, slot):
        return [pltpu.make_async_remote_copy(
            src_ref=src.at[d], dst_ref=dst.at[slot], send_sem=head_send_sem.at[kind, d],
            recv_sem=head_recv_sem.at[kind, slot], device_id={"fib": d}, device_id_type=MESH)
            for kind, (src, dst) in enumerate(((flux_send, flux_recv), (ivar_send, ivar_recv)))]

    def tail_copies(d, j, to, slot):
        return [pltpu.make_async_remote_copy(
            src_ref=src.at[d, j], dst_ref=dst.at[slot, j], send_sem=send_sem.at[kind, d, j],
            recv_sem=recv_sem.at[kind, slot, j], device_id={"fib": to}, device_id_type=MESH)
            for kind, (src, dst) in enumerate(((scale_send, scale_recv), (band_send, band_recv)))]

    def order(t):
        return peer(jnp.where(is_relay, lax.rem(t + 1, n_fib - 1), t))

    def send_tail(t, j):
        d = order(t)
        relayed = is_end & (t == 0)
        return tail_copies(d, j, jnp.where(relayed, relay, d), jnp.where(relayed, relay, me))

    def make_head(t, c):
        d = peer(t)
        ivar, flux = head(d)
        flux_send[d] = flux
        ivar_send[d] = (ivar * UNIT).astype(jnp.int32).astype(jnp.int16)
        return c

    lax.fori_loop(0, n_fib - 1, make_head, 0)
    band_load.wait()

    def sums(d, j):
        rows = pl.ds(pl.multiple_of(d * share + j * ROWS, ROWS), ROWS)
        w = [weight[e, rows, :] for e in range(exposures)]
        out = []
        for b in range(n_bands):
            total = w[0] * bands[0, b, rows, :].astype(f32)
            for e in range(1, exposures):
                total += w[e] * bands[e, b, rows, :].astype(f32)
            out.append(total)
        return out

    def pack(d, j, total):
        top = functools.reduce(jnp.maximum, total)
        scale = (jnp.maximum(top, TINY) * 1.01).astype(jnp.bfloat16)
        scale_send[d, j] = scale
        factor = TOP / scale.astype(f32)
        for b in range(n_bands):
            band_send[d, j, b] = (total[b] * factor + 0.5).astype(jnp.int32).astype(jnp.int16)

    def store(ref, j, total):
        for b in range(n_bands):
            ref[b, pl.ds(j * ROWS, ROWS), :] = total[b]

    for j in range(pieces):
        d = order(0)
        pack(d, j, sums(d, j))

    pl.semaphore_wait(barrier, n_fib + 1)

    def send_head(t, c):
        for copy in head_copies(peer(t), me):
            copy.start()
        return c

    lax.fori_loop(0, n_fib - 1, send_head, 0)
    for j in range(pieces):
        for copy in send_tail(0, j):
            copy.start()

    def make_bands(t, c):
        d = order(t)
        for j in range(pieces):
            pack(d, j, sums(d, j))
            for copy in send_tail(t, j):
                copy.start()
        return c

    lax.fori_loop(1, n_fib - 1 - jnp.where(is_relay, 1, 0), make_bands, 0)

    @pl.when(is_relay)
    def _():
        for j in range(pieces):
            store(held, j, sums(far, j))

    for j in range(pieces):
        store(own_band, j, sums(me, j))
    ivar, flux = head(me)

    @pl.when(is_relay)
    def _():
        for j in range(pieces):
            for copy in tail_copies(far, j, far, me):
                copy.wait_recv()
            scale = scale_recv[me, j].astype(f32) * (1.0 / TOP)
            pack(far, j, [held[b, pl.ds(j * ROWS, ROWS), :] + band_recv[me, j, b].astype(f32) * scale
                          for b in range(n_bands)])
            for copy in tail_copies(far, j, far, me):
                copy.start()

    def add_head(t, carry):
        ivar, flux = carry
        d = peer(n_fib - 2 - t)
        for copy in head_copies(d, d):
            copy.wait_recv()
        return ivar + ivar_recv[d].astype(f32) * (1.0 / UNIT), flux + flux_recv[d]

    ivar, flux = lax.fori_loop(0, n_fib - 1, add_head, (ivar, flux))
    inverse = 1.0 / ivar
    coadd = flux / ivar
    ivar_out[...] = ivar[None]
    flux_out[...] = coadd[None]
    flux_full[...] = coadd
    to_right = pltpu.make_async_remote_copy(
        src_ref=flux_full, dst_ref=side.at[0], send_sem=side_send_sem.at[0], recv_sem=side_recv_sem.at[0],
        device_id={"wav": right}, device_id_type=MESH)
    to_left = pltpu.make_async_remote_copy(
        src_ref=flux_full, dst_ref=side.at[1], send_sem=side_send_sem.at[1], recv_sem=side_recv_sem.at[1],
        device_id={"wav": left}, device_id_type=MESH)
    to_right.start()
    to_left.start()
    to_right.wait_recv()
    to_left.wait_recv()
    before = jnp.where(w_me == 0, 0.0, side[0])
    after = jnp.where(w_me == n_wav - 1, 0.0, side[1])
    lane = lax.broadcasted_iota(jnp.int32, (share, width), 1)
    for b in range(n_bands):
        shift = b - HALF
        if shift == 0:
            rolled[b] = coadd
        elif shift > 0:
            rolled[b] = pltpu.roll(jnp.where(lane >= shift, coadd, after), width - shift, 1)
        else:
            rolled[b] = pltpu.roll(jnp.where(lane < width + shift, coadd, before), -shift, 1)

    def add_bands(t, c):
        d = peer(jnp.where(is_relay, lax.rem(2 * n_fib - 4 - t, n_fib - 1), n_fib - 2 - t))
        for j in range(pieces):
            for copy in tail_copies(d, j, d, d):
                copy.wait_recv()
            scale = scale_recv[d, j].astype(f32) * (1.0 / TOP)
            for b in range(n_bands):
                own_band[b, pl.ds(j * ROWS, ROWS), :] += band_recv[d, j, b].astype(f32) * scale
        return c

    lax.fori_loop(0, n_fib - 1 - jnp.where(is_end, 1, 0), add_bands, 0)
    model = None
    for b in range(n_bands):
        res = own_band[b] * inverse
        res_out[0, b] = res
        term = res * rolled[b]
        model = term if model is None else model + term
    model_out[...] = model[None]

    def finish(t, c):
        d = peer(t)
        for copy in head_copies(d, me):
            copy.wait_send()
        for j in range(pieces):
            for copy in tail_copies(d, j, d, me):
                copy.wait_send()
        return c

    lax.fori_loop(0, n_fib - 1, finish, 0)
    to_right.wait_send()
    to_left.wait_send()


def write_out(*refs):
    half = len(refs) // 2
    sem = refs[-1]
    loads = [pltpu.make_async_copy(refs[i], refs[half + i], sem.at[i]) for i in range(half)]
    for copy in loads:
        copy.start()
    for copy in loads:
        copy.wait()


def local(n_fib, n_wav, spectra, bands, coverage):
    spectra, bands = spectra[:, 0], bands[:, 0]
    exposures, n_bands, fibers, width = bands.shape
    share = fibers // n_fib
    pieces = share // ROWS
    f32, i16, bf16 = jnp.float32, jnp.int16, jnp.bfloat16
    plane = jax.ShapeDtypeStruct((1, share, width), f32)
    vmem = pltpu.VMEM
    sem = pltpu.SemaphoreType.DMA
    shapes = (plane, plane, jax.ShapeDtypeStruct((1, n_bands, share, width), f32), plane)
    parts = pl.pallas_call(
        functools.partial(kernel, n_fib, n_wav),
        out_shape=tuple(vmem(x.shape, f32) for x in shapes),
        in_specs=[pl.BlockSpec(memory_space=pl.ANY)] * 3,
        out_specs=[pl.BlockSpec(memory_space=pltpu.VMEM)] * 4,
        scratch_shapes=[
            vmem(spectra.shape, bf16),
            vmem(bands.shape, bf16),
            vmem(coverage.shape, jnp.int32),
            vmem((exposures, fibers, width), f32),
            vmem((n_fib, share, width), f32),
            vmem((n_fib, share, width), i16),
            vmem((n_fib, pieces, ROWS, width), bf16),
            vmem((n_fib, pieces, n_bands, ROWS, width), i16),
            vmem((n_fib, share, width), f32),
            vmem((n_fib, share, width), i16),
            vmem((n_fib, pieces, ROWS, width), bf16),
            vmem((n_fib, pieces, n_bands, ROWS, width), i16),
            vmem((n_bands, share, width), f32),
            vmem((n_bands, share, width), f32),
            vmem((share, width), f32),
            vmem((2, share, width), f32),
            vmem((n_bands, share, width), f32),
            sem((3,)),
            sem((2, n_fib)),
            sem((2, n_fib)),
            sem((2, n_fib, pieces)),
            sem((2, n_fib, pieces)),
            sem((2,)),
            sem((2,)),
        ],
        compiler_params=pltpu.CompilerParams(collective_id=0, has_side_effects=True),
        name="coadd",
    )(spectra, bands, coverage)
    return pl.pallas_call(
        write_out,
        out_shape=shapes,
        in_specs=[pl.BlockSpec(memory_space=pltpu.VMEM)] * 4,
        out_specs=[pl.BlockSpec(memory_space=pl.ANY)] * 4,
        scratch_shapes=[sem((4,))],
        compiler_params=pltpu.CompilerParams(vmem_limit_bytes=4 * 2**20),
        name="write_out",
    )(*parts)


def solution(mesh):
    sizes = dict(mesh.shape)
    return jax.shard_map(
        functools.partial(local, sizes["fib"], sizes["wav"]),
        mesh=mesh,
        in_specs=(
            P(("grp", "fib"), "arm", None, None, "wav"),
            P(("grp", "fib"), "arm", None, None, "wav"),
            P(("grp", "fib"), None),
        ),
        out_specs=(
            P("arm", ("grp", "fib"), "wav"),
            P("arm", ("grp", "fib"), "wav"),
            P("arm", None, ("grp", "fib"), "wav"),
            P("arm", ("grp", "fib"), "wav"),
        ),
        check_vma=False,
    )
```

```python
import functools

import jax
import jax.numpy as jnp
from jax import lax
from jax.experimental import pallas as pl
from jax.experimental.pallas import tpu as pltpu
from jax.sharding import PartitionSpec as P

MESH = pl.DeviceIdType.MESH
HALF = 5
UNIT = 512.0
TOP = 32767.0
TINY = 1e-30
ROWS = 16


def kernel(n_fib, n_wav, spec_hbm, bands_hbm, cov_hbm, flux_out, ivar_out, res_out, model_out,
           spec, bands, cov, weight, flux_send, ivar_send, scale_send, band_send,
           flux_recv, ivar_recv, scale_recv, band_recv, own_band, held, flux_full, side, rolled,
           load_sem, head_send_sem, head_recv_sem, send_sem, recv_sem, side_send_sem, side_recv_sem):
    f32 = jnp.float32
    me = lax.axis_index("fib")
    w_me = lax.axis_index("wav")
    right, left = lax.rem(w_me + 1, n_wav), lax.rem(w_me + n_wav - 1, n_wav)
    exposures, n_bands, fibers, width = bands.shape
    share = fibers // n_fib

    cov_load = pltpu.make_async_copy(cov_hbm, cov, load_sem.at[0])
    spec_load = pltpu.make_async_copy(spec_hbm, spec, load_sem.at[1])
    band_load = pltpu.make_async_copy(bands_hbm, bands, load_sem.at[2])
    cov_load.start()
    spec_load.start()
    band_load.start()

    def peer(t):
        low = n_fib - 1 - t
        low = jnp.where(low <= me, low - 1, low)
        high = jnp.where(t >= me, t + 1, t)
        return jnp.where(2 * me < n_fib, low, high)

    barrier = pltpu.get_barrier_semaphore()

    def greet(t, c):
        pl.semaphore_signal(barrier, inc=1, device_id={"fib": peer(t)}, device_id_type=MESH)
        return c

    lax.fori_loop(0, n_fib - 1, greet, 0)
    pl.semaphore_signal(barrier, inc=1, device_id={"wav": right}, device_id_type=MESH)
    pl.semaphore_signal(barrier, inc=1, device_id={"wav": left}, device_id_type=MESH)

    cov_load.wait()
    spec_load.wait()

    seen = cov[...].astype(f32)
    for e in range(exposures):
        column = jnp.transpose(jnp.broadcast_to(seen[e : e + 1, :], (width, fibers)))
        weight[e] = spec[e, 1].astype(f32) * column

    pieces = share // ROWS
    is_end = (me == 0) | (me == n_fib - 1)
    is_relay = (me == 1) | (me == n_fib - 2)
    relay = jnp.where(me == 0, 1, n_fib - 2)
    far = jnp.where(me == 1, n_fib - 1, 0)

    def head(d):
        rows = pl.ds(pl.multiple_of(d * share, share), share)
        w = [weight[e, rows, :] for e in range(exposures)]
        ivar = w[0]
        flux = w[0] * spec[0, 0, rows, :].astype(f32)
        for e in range(1, exposures):
            ivar += w[e]
            flux += w[e] * spec[e, 0, rows, :].astype(f32)
        return ivar, flux

    def head_copies(d, slot):
        return [pltpu.make_async_remote_copy(
            src_ref=src.at[d], dst_ref=dst.at[slot], send_sem=head_send_sem.at[kind, d],
            recv_sem=head_recv_sem.at[kind, slot], device_id={"fib": d}, device_id_type=MESH)
            for kind, (src, dst) in enumerate(((flux_send, flux_recv), (ivar_send, ivar_recv)))]

    def tail_copies(d, j, to, slot):
        return [pltpu.make_async_remote_copy(
            src_ref=src.at[d, j], dst_ref=dst.at[slot, j], send_sem=send_sem.at[kind, d, j],
            recv_sem=recv_sem.at[kind, slot, j], device_id={"fib": to}, device_id_type=MESH)
            for kind, (src, dst) in enumerate(((scale_send, scale_recv), (band_send, band_recv)))]

    def order(t):
        turned = jnp.where(t == 0, 0, n_fib - 1 - t)
        return peer(jnp.where(is_relay, lax.rem(t + 1, n_fib - 1), jnp.where(is_end, turned, t)))

    def send_tail(t, j):
        d = order(t)
        relayed = is_end & (t == 0)
        return tail_copies(d, j, jnp.where(relayed, relay, d), jnp.where(relayed, relay, me))

    def make_head(t, c):
        d = peer(t)
        ivar, flux = head(d)
        flux_send[d] = flux
        ivar_send[d] = (ivar * UNIT).astype(jnp.int32).astype(jnp.int16)
        return c

    lax.fori_loop(0, n_fib - 1, make_head, 0)
    band_load.wait()

    def sums(d, j):
        rows = pl.ds(pl.multiple_of(d * share + j * ROWS, ROWS), ROWS)
        w = [weight[e, rows, :] for e in range(exposures)]
        out = []
        for b in range(n_bands):
            total = w[0] * bands[0, b, rows, :].astype(f32)
            for e in range(1, exposures):
                total += w[e] * bands[e, b, rows, :].astype(f32)
            out.append(total)
        return out

    def pack(d, j, total):
        top = functools.reduce(jnp.maximum, total)
        scale = (jnp.maximum(top, TINY) * 1.01).astype(jnp.bfloat16)
        scale_send[d, j] = scale
        factor = TOP / scale.astype(f32)
        for b in range(n_bands):
            band_send[d, j, b] = (total[b] * factor + 0.5).astype(jnp.int32).astype(jnp.int16)

    def store(ref, j, total):
        for b in range(n_bands):
            ref[b, pl.ds(j * ROWS, ROWS), :] = total[b]

    for j in range(pieces):
        d = order(0)
        pack(d, j, sums(d, j))

    pl.semaphore_wait(barrier, n_fib + 1)

    def send_head(t, c):
        for copy in head_copies(peer(t), me):
            copy.start()
        return c

    def send_first():
        for j in range(pieces):
            for copy in send_tail(0, j):
                copy.start()

    @pl.when(is_end)
    def _():
        send_first()

    lax.fori_loop(0, n_fib - 1, send_head, 0)

    @pl.when(jnp.logical_not(is_end))
    def _():
        send_first()


    def make_bands(t, c):
        d = order(t)
        for j in range(pieces):
            pack(d, j, sums(d, j))
            for copy in send_tail(t, j):
                copy.start()
        return c

    lax.fori_loop(1, n_fib - 1 - jnp.where(is_relay, 1, 0), make_bands, 0)

    @pl.when(is_relay)
    def _():
        for j in range(pieces):
            store(held, j, sums(far, j))

    for j in range(pieces):
        store(own_band, j, sums(me, j))
    ivar, flux = head(me)

    @pl.when(is_relay)
    def _():
        for j in range(pieces):
            for copy in tail_copies(far, j, far, me):
                copy.wait_recv()
            scale = scale_recv[me, j].astype(f32) * (1.0 / TOP)
            pack(far, j, [held[b, pl.ds(j * ROWS, ROWS), :] + band_recv[me, j, b].astype(f32) * scale
                          for b in range(n_bands)])
            for copy in tail_copies(far, j, far, me):
                copy.start()

    def add_head(t, carry):
        ivar, flux = carry
        d = peer(n_fib - 2 - t)
        for copy in head_copies(d, d):
            copy.wait_recv()
        return ivar + ivar_recv[d].astype(f32) * (1.0 / UNIT), flux + flux_recv[d]

    ivar, flux = lax.fori_loop(0, n_fib - 1, add_head, (ivar, flux))
    inverse = 1.0 / ivar
    coadd = flux / ivar
    ivar_out[...] = ivar[None]
    flux_out[...] = coadd[None]
    flux_full[...] = coadd
    to_right = pltpu.make_async_remote_copy(
        src_ref=flux_full, dst_ref=side.at[0], send_sem=side_send_sem.at[0], recv_sem=side_recv_sem.at[0],
        device_id={"wav": right}, device_id_type=MESH)
    to_left = pltpu.make_async_remote_copy(
        src_ref=flux_full, dst_ref=side.at[1], send_sem=side_send_sem.at[1], recv_sem=side_recv_sem.at[1],
        device_id={"wav": left}, device_id_type=MESH)
    to_right.start()
    to_left.start()
    to_right.wait_recv()
    to_left.wait_recv()
    before = jnp.where(w_me == 0, 0.0, side[0])
    after = jnp.where(w_me == n_wav - 1, 0.0, side[1])
    lane = lax.broadcasted_iota(jnp.int32, (share, width), 1)
    for b in range(n_bands):
        shift = b - HALF
        if shift == 0:
            rolled[b] = coadd
        elif shift > 0:
            rolled[b] = pltpu.roll(jnp.where(lane >= shift, coadd, after), width - shift, 1)
        else:
            rolled[b] = pltpu.roll(jnp.where(lane < width + shift, coadd, before), -shift, 1)

    def add_bands(t, c):
        d = peer(jnp.where(is_relay, lax.rem(2 * n_fib - 4 - t, n_fib - 1), n_fib - 2 - t))
        for j in range(pieces):
            for copy in tail_copies(d, j, d, d):
                copy.wait_recv()
            scale = scale_recv[d, j].astype(f32) * (1.0 / TOP)
            for b in range(n_bands):
                own_band[b, pl.ds(j * ROWS, ROWS), :] += band_recv[d, j, b].astype(f32) * scale
        return c

    lax.fori_loop(0, n_fib - 1 - jnp.where(is_end, 1, 0), add_bands, 0)
    model = None
    for b in range(n_bands):
        res = own_band[b] * inverse
        res_out[0, b] = res
        term = res * rolled[b]
        model = term if model is None else model + term
    model_out[...] = model[None]

    def finish(t, c):
        d = peer(t)
        for copy in head_copies(d, me):
            copy.wait_send()
        for j in range(pieces):
            for copy in tail_copies(d, j, d, me):
                copy.wait_send()
        return c

    lax.fori_loop(0, n_fib - 1, finish, 0)
    to_right.wait_send()
    to_left.wait_send()


def write_out(*refs):
    half = len(refs) // 2
    sem = refs[-1]
    loads = [pltpu.make_async_copy(refs[i], refs[half + i], sem.at[i]) for i in range(half)]
    for copy in loads:
        copy.start()
    for copy in loads:
        copy.wait()


def local(n_fib, n_wav, spectra, bands, coverage):
    spectra, bands = spectra[:, 0], bands[:, 0]
    exposures, n_bands, fibers, width = bands.shape
    share = fibers // n_fib
    pieces = share // ROWS
    f32, i16, bf16 = jnp.float32, jnp.int16, jnp.bfloat16
    plane = jax.ShapeDtypeStruct((1, share, width), f32)
    vmem = pltpu.VMEM
    sem = pltpu.SemaphoreType.DMA
    shapes = (plane, plane, jax.ShapeDtypeStruct((1, n_bands, share, width), f32), plane)
    parts = pl.pallas_call(
        functools.partial(kernel, n_fib, n_wav),
        out_shape=tuple(vmem(x.shape, f32) for x in shapes),
        in_specs=[pl.BlockSpec(memory_space=pl.ANY)] * 3,
        out_specs=[pl.BlockSpec(memory_space=pltpu.VMEM)] * 4,
        scratch_shapes=[
            vmem(spectra.shape, bf16),
            vmem(bands.shape, bf16),
            vmem(coverage.shape, jnp.int32),
            vmem((exposures, fibers, width), f32),
            vmem((n_fib, share, width), f32),
            vmem((n_fib, share, width), i16),
            vmem((n_fib, pieces, ROWS, width), bf16),
            vmem((n_fib, pieces, n_bands, ROWS, width), i16),
            vmem((n_fib, share, width), f32),
            vmem((n_fib, share, width), i16),
            vmem((n_fib, pieces, ROWS, width), bf16),
            vmem((n_fib, pieces, n_bands, ROWS, width), i16),
            vmem((n_bands, share, width), f32),
            vmem((n_bands, share, width), f32),
            vmem((share, width), f32),
            vmem((2, share, width), f32),
            vmem((n_bands, share, width), f32),
            sem((3,)),
            sem((2, n_fib)),
            sem((2, n_fib)),
            sem((2, n_fib, pieces)),
            sem((2, n_fib, pieces)),
            sem((2,)),
            sem((2,)),
        ],
        compiler_params=pltpu.CompilerParams(collective_id=0, has_side_effects=True),
        name="coadd",
    )(spectra, bands, coverage)
    return pl.pallas_call(
        write_out,
        out_shape=shapes,
        in_specs=[pl.BlockSpec(memory_space=pltpu.VMEM)] * 4,
        out_specs=[pl.BlockSpec(memory_space=pl.ANY)] * 4,
        scratch_shapes=[sem((4,))],
        compiler_params=pltpu.CompilerParams(vmem_limit_bytes=4 * 2**20),
        name="write_out",
    )(*parts)


def solution(mesh):
    sizes = dict(mesh.shape)
    return jax.shard_map(
        functools.partial(local, sizes["fib"], sizes["wav"]),
        mesh=mesh,
        in_specs=(
            P(("grp", "fib"), "arm", None, None, "wav"),
            P(("grp", "fib"), "arm", None, None, "wav"),
            P(("grp", "fib"), None),
        ),
        out_specs=(
            P("arm", ("grp", "fib"), "wav"),
            P("arm", ("grp", "fib"), "wav"),
            P("arm", None, ("grp", "fib"), "wav"),
            P("arm", ("grp", "fib"), "wav"),
        ),
        check_vma=False,
    )
```
